32 devices in a mesh: fsdp: 16 (over z, x, core), tp: 2 (over y).
Axes of the slice: x: 2, y: 2, z: 4, core: 2. Of those that a mesh axis runs over, the one named last changes fastest.
Arguments:
- saved_master: float32 [16384, 5120], P(('fsdp', 'tp')), may hold values from -6 to 6
- saved_first: float32 [16384, 5120], P(('fsdp', 'tp')), may hold values from -6 to 6
- saved_second: float32 [16384, 5120], P(('fsdp', 'tp')), may hold values from 0.05 to 20
- grad: bfloat16 [16384, 5120], P('fsdp', 'tp'), may hold values from -10000 to 10000
- row_target: int32 [16384], replicated, may hold values from 0 to 16383, as said below
- step: int32 [1], replicated, may hold values from 1 to 63
Outputs:
- new_master: float32 [16384, 5120], P('fsdp', 'tp')
- new_first: float32 [16384, 5120], P('fsdp', 'tp')
- new_second: float32 [16384, 5120], P('fsdp', 'tp')
- direction: float32 [16384, 5120], P('fsdp', 'tp')
The draws below stay inside these ranges and needn't reach their ends.
Inputs may be any that keep to these rules, and one draw needn't show every extreme that they name: `row_target`: a permutation of 0 to 16383; the saved rows j * 1024 to (j + 1) * 1024 - 1 of every block j send exactly 64 rows into every new block of 1024 rows.
All inputs are finite; a program needn't handle non-finite values.
Results may differ from the reference program's by a relative error of at most 0.0003.
Values sent between devices are 32-bit elements; how exact they have to be, the bound alone decides.
A program may use at most 192 MiB of HBM per device.

```python
import math
import jax
import jax.numpy as jnp

H = 16384
D = 5120
N_FSDP = 16


def draw_row_target(key, part):
    block_rows = H // N_FSDP
    pair_rows = block_rows // N_FSDP
    source_keys = jax.random.split(jax.random.fold_in(key, 11), N_FSDP)
    target_keys = jax.random.split(jax.random.fold_in(key, 12), N_FSDP)
    sigma = jax.vmap(lambda one: jax.random.permutation(one, block_rows))(source_keys).astype(jnp.int32)
    tau_table = jax.vmap(lambda one: jax.random.permutation(one, block_rows))(target_keys).astype(jnp.int32)
    target_block = sigma // pair_rows
    slot_index = sigma % pair_rows
    incoming = jnp.arange(N_FSDP, dtype=jnp.int32)[:, None] * pair_rows + slot_index
    local_row = tau_table.reshape(-1)[target_block * block_rows + incoming]
    return (target_block * block_rows + local_row).reshape(-1).astype(jnp.int32)


def draw_grad(key, part):
    row_key = jax.random.fold_in(key, 21)
    col_key = jax.random.fold_in(key, 22)
    base_key = jax.random.fold_in(key, 23)
    rising = 1.0 + 2.0 * jnp.arange(H, dtype=jnp.float32) / (H - 1)
    row_scale = jnp.exp(jax.random.uniform(row_key, (H, 1)) * math.log(10.0)) * rising[:, None]
    col_scale = jnp.exp(jax.random.uniform(col_key, (1, D)) * math.log(10.0))
    values = jax.random.normal(base_key, (H, D))
    return (values * row_scale * col_scale).astype(jnp.bfloat16)


def level_of(key, extent, cuts, low, largest):
    factor_of, own = 1.0, jax.random.fold_in(key, 6)
    for position, shards_of in cuts:
        heights = jnp.exp(jax.random.uniform(jax.random.fold_in(own, position), (shards_of,), jnp.float32, low / len(cuts), largest / len(cuts)))
        factor_of = factor_of * jnp.repeat(heights, extent[position] // shards_of).reshape([-1 if axis == position else 1 for axis in range(len(extent))])
    return factor_of


def scatter_about(stream_key, dims, deviation, reach, cuts=(), kind=jnp.bfloat16):
    array = jax.random.normal(stream_key, dims, jnp.float32) * deviation
    if len(cuts) > 0:
        array = level_of(stream_key, dims, cuts, -0.22, 0.18) * array
    return jnp.clip(array, min=-reach, max=reach).astype(kind)


def setup_inputs(seed: int = 0) -> dict:
    key_list = jax.random.split(jax.random.key(seed), 7)
    saved_master = scatter_about(key_list[0], (H, D), 1.0, 6.0, ((0, 32),), jnp.float32)
    saved_first = scatter_about(key_list[1], (H, D), 1.0, 6.0, ((0, 32),), jnp.float32)
    saved_second = jnp.clip(jnp.exp(math.log(20.0) - 5.9914645 * jax.random.uniform(key_list[2], (H, D), jnp.float32) ** level_of(key_list[2], (H, D), ((0, 32),), -0.2, 0.2)), 0.05, 20.0)
    grad = draw_grad(jax.random.fold_in(key_list[6], 71), 0)
    row_target = draw_row_target(jax.random.fold_in(key_list[6], 71), 0)
    step = jax.random.randint(key_list[5], (1,), 1, 64).astype(jnp.int32)
    return dict(saved_master=saved_master, saved_first=saved_first, saved_second=saved_second, grad=grad, row_target=row_target, step=step)


beta_one = 0.9
beta_two = 0.95
epsilon = 1e-08
learn_rate = 0.001
weight_decay = 0.1

def adam_update(master, first, second, grad, scale, step):
    clipped = scale * grad.astype(jnp.float32)
    first_new = beta_one * first + (1.0 - beta_one) * clipped
    second_new = beta_two * second + (1.0 - beta_two) * clipped * clipped
    count = step[0].astype(jnp.float32)
    first_hat = first_new / (1.0 - jnp.power(jnp.float32(beta_one), count))
    second_hat = second_new / (1.0 - jnp.power(jnp.float32(beta_two), count))
    direction = first_hat / (jnp.sqrt(second_hat) + epsilon) + weight_decay * master
    return (master - learn_rate * direction, first_new, second_new, direction)

def reference(saved_master, saved_first, saved_second, grad, row_target, step):
    master = jnp.zeros_like(saved_master).at[row_target].set(saved_master)
    first = jnp.zeros_like(saved_first).at[row_target].set(saved_first)
    second = jnp.zeros_like(saved_second).at[row_target].set(saved_second)
    grad_wide = grad.astype(jnp.float32)
    total = jnp.sum(grad_wide * grad_wide)
    scale = jnp.minimum(1.0, math.sqrt(H * D) / jnp.sqrt(total))
    return adam_update(master, first, second, grad, scale, step)
```

```python
import math

import jax
import jax.numpy as jnp
from jax import lax
from jax.experimental import pallas as pl
from jax.experimental.pallas import tpu as pltpu
from jax.sharding import PartitionSpec as P

beta_one = 0.9
beta_two = 0.95
epsilon = 1e-08
learn_rate = 0.001
weight_decay = 0.1

LANES = 128
STAGES = 2
SENDS = 3
ARRIVALS = 4
SLOT = 1 << 12
MESH = pl.DeviceIdType.MESH


def partner_steps(count):
    bits = count.bit_length() - 1
    if 1 << bits != count:
        return list(range(1, count))
    return [int(format(i, f"0{bits}b")[::-1], 2) for i in range(1, count)]


def restore_kernel(
    count,
    entries,
    send_idx,
    place_idx,
    fixes,
    master_ref,
    first_ref,
    second_ref,
    grad_ref,
    out,
    landed,
    stage,
    send,
    recv_0,
    recv_1,
    recv_2,
    recv_3,
    grad,
    partial,
    partial_row,
    from_tp,
    from_fsdp,
    scale_ref,
    tp_sent,
    tp_landed,
    staged,
    sent,
    arrived,
    grad_sem,
    partial_sems,
):
    tp_count, fsdp_count = count
    f, t = lax.axis_index("fsdp"), lax.axis_index("tp")
    saved = (master_ref, first_ref, second_ref)
    arrivals = (recv_0, recv_1, recv_2, recv_3)
    steps, block_rows = out.shape[1], out.shape[2]
    columns = steps * LANES
    piece = master_ref.shape[0]
    pair = block_rows // fsdp_count
    power = fsdp_count & (fsdp_count - 1) == 0

    def along_tp(d):
        return lax.rem(t + d, tp_count)

    def along_fsdp(d):
        return jnp.bitwise_xor(f, d) if power else lax.rem(f + d, fsdp_count)

    def unit(ref, half, s):
        return ref.at[:, pl.ds(pl.multiple_of(half * columns + s * LANES, LANES), LANES)]

    def tp_start(s):
        for d in range(1, tp_count):
            peer = along_tp(d)
            for x, ref in enumerate(saved):
                pltpu.make_async_remote_copy(
                    src_ref=unit(ref, peer, s),
                    dst_ref=landed.at[s, t, x],
                    send_sem=tp_sent.at[s],
                    recv_sem=tp_landed.at[s],
                    device_id=(f, peer),
                    device_id_type=MESH,
                ).start()

    def tp_wait(s, sem):
        if tp_count > 1:
            whole = landed.at[s, pl.ds(0, tp_count - 1)]
            pltpu.make_async_copy(whole, whole, sem.at[s]).wait()

    def stage_start(s):
        slot = lax.rem(s, STAGES)
        for d in range(tp_count):
            half = along_tp(d)
            for x, ref in enumerate(saved):
                rows = pl.ds(pl.multiple_of((half * 3 + x) * piece, 8), piece)
                source = unit(ref, t, s) if d == 0 else landed.at[s, half, x]
                pltpu.make_async_copy(source, stage.at[slot, rows], staged.at[slot]).start()

    def stage_wait(s):
        slot = lax.rem(s, STAGES)
        pltpu.make_async_copy(stage.at[slot], stage.at[slot], staged.at[slot]).wait()

    def with_arrival(s, body):
        for i, recv in enumerate(arrivals):
            pl.when(lax.rem(s, len(arrivals)) == i)(lambda recv=recv: body(s, recv))

    def send_start(s, recv):
        slot = lax.rem(s, SENDS)
        recv[f] = send[slot, f]
        for d in partner_steps(fsdp_count):
            peer = along_fsdp(d)
            pltpu.make_async_remote_copy(
                src_ref=send.at[slot, peer],
                dst_ref=recv.at[f],
                send_sem=sent.at[slot],
                recv_sem=arrived.at[s],
                device_id=(peer, t),
                device_id_type=MESH,
            ).start()

    def send_wait(s):
        slot = lax.rem(s, SENDS)
        whole = send.at[slot, pl.ds(0, fsdp_count - 1)]
        pltpu.make_async_copy(whole, whole, sent.at[slot]).wait()

    def recv_wait(s):
        whole = send.at[0, pl.ds(0, fsdp_count - 1)]
        pltpu.make_async_copy(whole, whole, arrived.at[s]).wait()

    run = math.gcd(pair, 8)

    def gather(s):
        source, slot = lax.rem(s, STAGES), lax.rem(s, SENDS)

        def one_block(b, carry):
            def one_run(k, carry):
                for u in range(run):
                    row = send_idx[b * pair + k * run + u]
                    for x in range(3):
                        send[slot, b, pl.ds(x * pair + k * run + u, 1), :] = stage[
                            source, pl.ds(row + x * piece, 1), :
                        ]
                return carry

            return lax.fori_loop(0, pair // run, one_run, carry)

        lax.fori_loop(0, fsdp_count, one_block, 0)

    def place(s, recv):

        def one_run(k, carry):
            for u in range(8):
                packed = place_idx[k * 8 + u]
                block, row = packed // SLOT, packed % SLOT
                for x in range(3):
                    out[x, s, pl.ds(k * 8 + u, 1), :] = recv[block, pl.ds(row + x * pair, 1), :]
            return carry

        lax.fori_loop(0, block_rows // 8, one_run, 0)

    tile = math.gcd(block_rows, 64)

    def adam(s):
        scale = scale_ref[...]
        first_fix, second_fix = fixes[0], fixes[1]

        def one_tile(k, carry):
            rows = pl.ds(pl.multiple_of(k * tile, tile), tile)
            clipped = scale * grad[s, rows, :].astype(jnp.float32)
            master = out[0, s, rows, :]
            first_new = beta_one * out[1, s, rows, :] + (1.0 - beta_one) * clipped
            second_new = beta_two * out[2, s, rows, :] + (1.0 - beta_two) * clipped * clipped
            first_hat = first_new / first_fix
            second_hat = second_new / second_fix
            direction = first_hat / (jnp.sqrt(second_hat) + epsilon) + weight_decay * master
            out[0, s, rows, :] = master - learn_rate * direction
            out[1, s, rows, :] = first_new
            out[2, s, rows, :] = second_new
            out[3, s, rows, :] = direction
            return carry

        lax.fori_loop(0, block_rows // tile, one_tile, 0)

    def square_sum():
        def one_unit(s, total):
            def one_tile(k, total):
                rows = pl.ds(pl.multiple_of(k * tile, tile), tile)
                wide = grad[s, rows, :].astype(jnp.float32)
                return total + wide * wide

            return lax.fori_loop(0, block_rows // tile, one_tile, total)

        total = lax.fori_loop(0, steps, one_unit, jnp.zeros((tile, LANES), jnp.float32))
        return jnp.sum(total, axis=0, keepdims=True)

    def partial_copies(which):
        if which == 0:
            peers = [(f, along_tp(d)) for d in range(1, tp_count)]
            source, target = partial, from_tp.at[t]
        else:
            peers = [(along_fsdp(d), t) for d in partner_steps(fsdp_count)]
            source, target = partial_row, from_fsdp.at[f]
        return [
            pltpu.make_async_remote_copy(
                src_ref=source,
                dst_ref=target,
                send_sem=partial_sems.at[2 * which],
                recv_sem=partial_sems.at[2 * which + 1],
                device_id=peer,
                device_id_type=MESH,
            )
            for peer in peers
        ]

    def partial_wait(which, side):
        held = (from_tp, from_fsdp)[which]
        members = (tp_count, fsdp_count)[which]
        if members > 1:
            whole = held.at[pl.ds(0, members - 1)]
            pltpu.make_async_copy(whole, whole, partial_sems.at[2 * which + side]).wait()

    def summed(held, members):
        total = held[0]
        for i in range(1, members):
            total = total + held[i]
        return total

    def grad_copy(s):
        return pltpu.make_async_copy(unit(grad_ref, 0, s), grad.at[s], grad_sem)

    tp_start(0)
    lax.fori_loop(0, steps, lambda s, carry: (grad_copy(s).start(), carry)[1], 0)
    pltpu.make_async_copy(grad, grad, grad_sem).wait()
    own = square_sum()
    partial[...] = own
    from_tp[t] = own
    for copy in partial_copies(0):
        copy.start()
    if steps > 1:
        tp_start(1)
    tp_wait(0, tp_landed)
    stage_start(0)

    def step(s, carry):
        @pl.when(s < steps)
        def _():
            stage_wait(s)

            @pl.when(s >= SENDS)
            def _():
                send_wait(s - SENDS)

            gather(s)
            with_arrival(s, send_start)

            @pl.when(s == 0)
            def _():
                partial_wait(0, 1)
                row = summed(from_tp, tp_count)
                partial_row[...] = row
                from_fsdp[f] = row
                for copy in partial_copies(1):
                    copy.start()

            @pl.when(s + 2 < steps)
            def _():
                tp_start(s + 2)

            @pl.when(s + 1 < steps)
            def _():
                tp_wait(s + 1, tp_landed)
                stage_start(s + 1)

        @pl.when(s >= 1)
        def _():
            recv_wait(s - 1)
            with_arrival(s - 1, place)

            @pl.when(s == 1)
            def _():
                partial_wait(1, 1)
                total = jnp.sum(summed(from_fsdp, fsdp_count), axis=1, keepdims=True)
                scale = jnp.minimum(1.0, math.sqrt(entries) / jnp.sqrt(total))
                scale_ref[...] = jnp.broadcast_to(scale, scale_ref.shape)

            adam(s - 1)

        return carry

    lax.fori_loop(0, steps + 1, step, 0)
    for s in range(max(0, steps - SENDS), steps):
        send_wait(s)
    lax.fori_loop(0, steps, lambda s, carry: (tp_wait(s, tp_sent), carry)[1], 0)
    partial_wait(0, 0)
    partial_wait(1, 0)


def drain_kernel(held, *refs):
    outs, sem = refs[:-1], refs[-1]
    copies = [
        pltpu.make_async_copy(
            held.at[i, u], out.at[:, u * LANES : (u + 1) * LANES], sem.at[i, u]
        )
        for i, out in enumerate(outs)
        for u in range(held.shape[1])
    ]
    for copy in copies:
        copy.start()
    for copy in copies:
        copy.wait()


def per_device(entries, saved_master, saved_first, saved_second, grad, row_target, step):
    tp_count, fsdp_count = lax.axis_size("tp"), lax.axis_size("fsdp")
    block_index = lax.axis_index("fsdp")
    block_rows, columns = grad.shape
    piece = saved_master.shape[0]
    all_rows = row_target.shape[0]
    pair = block_rows // fsdp_count
    steps = columns // LANES

    mine = lax.dynamic_slice_in_dim(row_target, block_index * block_rows, block_rows)
    send_order = jnp.argsort(mine, stable=True).astype(jnp.int32)
    send_idx = (send_order // piece) * (3 * piece) + send_order % piece

    in_block = row_target // block_rows == block_index
    sort_keys = jnp.where(in_block, row_target, all_rows)
    source_block = jnp.argsort(sort_keys, stable=True)[:block_rows].astype(jnp.int32) // block_rows
    local = jnp.arange(block_rows, dtype=jnp.int32)
    before = (source_block[None, :] == source_block[:, None]) & (local[None, :] < local[:, None])
    place_idx = source_block * SLOT + jnp.sum(before.astype(jnp.int32), axis=1)

    taken = step[0].astype(jnp.float32)
    fixes = jnp.stack(
        [
            1.0 - jnp.power(jnp.float32(beta_one), taken),
            1.0 - jnp.power(jnp.float32(beta_two), taken),
        ]
    )

    def kernel(*refs):
        restore_kernel((tp_count, fsdp_count), entries, *refs)

    smem = pl.BlockSpec(memory_space=pltpu.SMEM)
    hbm = pl.BlockSpec(memory_space=pltpu.HBM)
    vmem = pl.BlockSpec(memory_space=pltpu.VMEM)
    dma = pltpu.SemaphoreType.DMA
    wide = jnp.float32
    held, _ = pl.pallas_call(
        kernel,
        out_shape=[
            pltpu.VMEM((4, steps, block_rows, LANES), wide),
            jax.ShapeDtypeStruct((steps, tp_count, 3, piece, LANES), wide),
        ],
        in_specs=[smem] * 3 + [hbm] * 4,
        out_specs=[vmem, hbm],
        scratch_shapes=[
            pltpu.VMEM((STAGES, tp_count * 3 * piece, LANES), wide),
            pltpu.VMEM((SENDS, fsdp_count, 3 * pair, LANES), wide),
        ]
        + [pltpu.VMEM((fsdp_count, 3 * pair, LANES), wide)] * ARRIVALS
        + [
            pltpu.VMEM((steps, block_rows, LANES), grad.dtype),
            pltpu.VMEM((1, LANES), wide),
            pltpu.VMEM((1, LANES), wide),
            pltpu.VMEM((tp_count, 1, LANES), wide),
            pltpu.VMEM((fsdp_count, 1, LANES), wide),
            pltpu.VMEM((1, LANES), wide),
            dma((steps,)),
            dma((steps,)),
            dma((STAGES,)),
            dma((SENDS,)),
            dma((steps,)),
            dma,
            dma((4,)),
        ],
        compiler_params=pltpu.CompilerParams(
            has_side_effects=True, vmem_limit_bytes=22 << 20
        ),
        name="restore",
    )(send_idx, place_idx, fixes, saved_master, saved_first, saved_second, grad)

    out = jax.ShapeDtypeStruct((block_rows, columns), wide)
    return tuple(
        pl.pallas_call(
            drain_kernel,
            out_shape=[out] * 4,
            in_specs=[pl.BlockSpec(memory_space=pl.ANY)],
            out_specs=[hbm] * 4,
            scratch_shapes=[dma((4, steps))],
            compiler_params=pltpu.CompilerParams(vmem_limit_bytes=1 << 20),
            name="drain",
        )(held)
    )


def solution(mesh):
    in_specs = (
        P(("fsdp", "tp"), None),
        P(("fsdp", "tp"), None),
        P(("fsdp", "tp"), None),
        P("fsdp", "tp"),
        P(),
        P(),
    )
    out_specs = (P("fsdp", "tp"), P("fsdp", "tp"), P("fsdp", "tp"), P("fsdp", "tp"))

    def whole(saved_master, saved_first, saved_second, grad, row_target, step):
        def body(*args):
            return per_device(grad.shape[0] * grad.shape[1], *args)

        return jax.shard_map(
            body, mesh=mesh, in_specs=in_specs, out_specs=out_specs, check_vma=False
        )(saved_master, saved_first, saved_second, grad, row_target, step)

    return whole
```

```python
import math

import jax
import jax.numpy as jnp
from jax import lax
from jax.experimental import pallas as pl
from jax.experimental.pallas import tpu as pltpu
from jax.sharding import PartitionSpec as P

beta_one = 0.9
beta_two = 0.95
epsilon = 1e-08
learn_rate = 0.001
weight_decay = 0.1

LANES = 128
SENDS = 2
ARRIVALS = 3
MESH = pl.DeviceIdType.MESH


def partner_steps(count):
    bits = count.bit_length() - 1
    if 1 << bits != count:
        return list(range(1, count))
    return [int(format(i, f"0{bits}b")[::-1], 2) for i in range(1, count)]


def restore_kernel(count, entries, *refs):
    tp_count, fsdp_count = count
    send_idx, place_idx, fixes, master_ref, first_ref, second_ref, grad_ref = refs[:7]
    out, landed = refs[7:9]
    stages, send = refs[9:12], refs[12]
    arrivals = [refs[13 + 3 * i : 16 + 3 * i] for i in range(ARRIVALS)]
    grad, partial, partial_row, from_tp, from_fsdp, scale_ref = refs[-13:-7]
    tp_sent, tp_landed, staged, sent, arrived, grad_sem, partial_sems = refs[-7:]
    f, t = lax.axis_index("fsdp"), lax.axis_index("tp")
    saved = (master_ref, first_ref, second_ref)
    steps, block_rows = out.shape[1], out.shape[2]
    columns = steps * LANES
    piece = master_ref.shape[0]
    pair = block_rows // fsdp_count
    power = fsdp_count & (fsdp_count - 1) == 0
    flat = pair % 8 == 0

    def along_tp(d):
        return lax.rem(t + d, tp_count)

    def along_fsdp(d):
        return jnp.bitwise_xor(f, d) if power else lax.rem(f + d, fsdp_count)

    def unit(ref, half, s):
        return ref.at[:, pl.ds(pl.multiple_of(half * columns + s * LANES, LANES), LANES)]

    def tp_start(s, x):
        for d in range(1, tp_count):
            peer = along_tp(d)
            pltpu.make_async_remote_copy(
                src_ref=unit(saved[x], peer, s),
                dst_ref=landed.at[s, x, t],
                send_sem=tp_sent.at[s, x],
                recv_sem=tp_landed.at[s, x],
                device_id=(f, peer),
                device_id_type=MESH,
            ).start()

    def tp_wait(s, x, sem):
        if tp_count > 1:
            whole = landed.at[s, x, pl.ds(0, tp_count - 1)]
            pltpu.make_async_copy(whole, whole, sem.at[s, x]).wait()

    def stage_start(s, x):
        for d in range(tp_count):
            half = along_tp(d)
            rows = pl.ds(pl.multiple_of(half * piece, 8), piece)
            source = unit(saved[x], t, s) if d == 0 else landed.at[s, x, half]
            pltpu.make_async_copy(source, stages[x].at[rows], staged.at[x]).start()

    def stage_wait(x):
        pltpu.make_async_copy(stages[x], stages[x], staged.at[x]).wait()

    def with_arrival(s, x, body):
        for i, held in enumerate(arrivals):
            pl.when(lax.rem(s, ARRIVALS) == i)(lambda recv=held[x]: body(s, x, recv))

    def block_of(recv, b):
        return pl.ds(pl.multiple_of(b * pair, 8), pair) if flat else b

    def send_start(s, x, recv):
        slot = lax.rem(s, SENDS)
        recv[block_of(recv, f)] = send[slot, x, f]
        for d in partner_steps(fsdp_count):
            peer = along_fsdp(d)
            pltpu.make_async_remote_copy(
                src_ref=send.at[slot, x, peer],
                dst_ref=recv.at[block_of(recv, f)],
                send_sem=sent.at[slot, x],
                recv_sem=arrived.at[s, x],
                device_id=(peer, t),
                device_id_type=MESH,
            ).start()

    def exchanged():
        return send.at[0, 0, pl.ds(0, fsdp_count - 1)]

    def send_wait(s, x):
        pltpu.make_async_copy(exchanged(), exchanged(), sent.at[lax.rem(s, SENDS), x]).wait()

    def recv_wait(s, x):
        pltpu.make_async_copy(exchanged(), exchanged(), arrived.at[s, x]).wait()

    run = math.gcd(pair, 8)

    def gather(s, x):
        slot = lax.rem(s, SENDS)

        def one_block(b, carry):
            def one_run(k, carry):
                for u in range(run):
                    row = send_idx[b * pair + k * run + u]
                    send[slot, x, b, pl.ds(k * run + u, 1), :] = stages[x][pl.ds(row, 1), :]
                return carry

            return lax.fori_loop(0, pair // run, one_run, carry)

        lax.fori_loop(0, fsdp_count, one_block, 0)

    def place(s, x, recv):
        def one_run(k, carry):
            for u in range(8):
                index = place_idx[k * 8 + u]
                if flat:
                    row = recv[pl.ds(index, 1), :]
                else:
                    row = recv[index // pair, pl.ds(index % pair, 1), :]
                out[x, s, pl.ds(k * 8 + u, 1), :] = row
            return carry

        lax.fori_loop(0, block_rows // 8, one_run, 0)

    tile = math.gcd(block_rows, 64)

    def adam(s):
        scale = scale_ref[...]
        first_fix, second_fix = fixes[0], fixes[1]

        def one_tile(k, carry):
            rows = pl.ds(pl.multiple_of(k * tile, tile), tile)
            clipped = scale * grad[s, rows, :].astype(jnp.float32)
            master = out[0, s, rows, :]
            first_new = beta_one * out[1, s, rows, :] + (1.0 - beta_one) * clipped
            second_new = beta_two * out[2, s, rows, :] + (1.0 - beta_two) * clipped * clipped
            first_hat = first_new / first_fix
            second_hat = second_new / second_fix
            direction = first_hat / (jnp.sqrt(second_hat) + epsilon) + weight_decay * master
            out[0, s, rows, :] = master - learn_rate * direction
            out[1, s, rows, :] = first_new
            out[2, s, rows, :] = second_new
            out[3, s, rows, :] = direction
            return carry

        lax.fori_loop(0, block_rows // tile, one_tile, 0)

    def square_sum():
        def one_unit(s, total):
            def one_tile(k, total):
                rows = pl.ds(pl.multiple_of(k * tile, tile), tile)
                wide = grad[s, rows, :].astype(jnp.float32)
                return total + wide * wide

            return lax.fori_loop(0, block_rows // tile, one_tile, total)

        total = lax.fori_loop(0, steps, one_unit, jnp.zeros((tile, LANES), jnp.float32))
        return jnp.sum(total, axis=0, keepdims=True)

    def partial_copies(which):
        if which == 0:
            peers = [(f, along_tp(d)) for d in range(1, tp_count)]
            source, target = partial, from_tp.at[t]
        else:
            peers = [(along_fsdp(d), t) for d in partner_steps(fsdp_count)]
            source, target = partial_row, from_fsdp.at[f]
        return [
            pltpu.make_async_remote_copy(
                src_ref=source,
                dst_ref=target,
                send_sem=partial_sems.at[2 * which],
                recv_sem=partial_sems.at[2 * which + 1],
                device_id=peer,
                device_id_type=MESH,
            )
            for peer in peers
        ]

    def partial_wait(which, side):
        held = (from_tp, from_fsdp)[which]
        members = (tp_count, fsdp_count)[which]
        if members > 1:
            whole = held.at[pl.ds(0, members - 1)]
            pltpu.make_async_copy(whole, whole, partial_sems.at[2 * which + side]).wait()

    def summed(held, members):
        total = held[0]
        for i in range(1, members):
            total = total + held[i]
        return total

    def grad_copy(s):
        return pltpu.make_async_copy(unit(grad_ref, 0, s), grad.at[s], grad_sem)

    def over_steps(body):
        lax.fori_loop(0, steps, lambda s, carry: (body(s), carry)[1], 0)

    for x in range(3):
        tp_start(0, x)
    over_steps(lambda s: grad_copy(s).start())
    tp_wait(0, 0, tp_landed)
    stage_start(0, 0)

    def begin_total():
        pltpu.make_async_copy(grad, grad, grad_sem).wait()
        own = square_sum()
        partial[...] = own
        from_tp[t] = own
        for copy in partial_copies(0):
            copy.start()

    def spread_total():
        partial_wait(0, 1)
        row = summed(from_tp, tp_count)
        partial_row[...] = row
        from_fsdp[f] = row
        for copy in partial_copies(1):
            copy.start()

    def end_total():
        partial_wait(1, 1)
        total = jnp.sum(summed(from_fsdp, fsdp_count), axis=1, keepdims=True)
        scale = jnp.minimum(1.0, math.sqrt(entries) / jnp.sqrt(total))
        scale_ref[...] = jnp.broadcast_to(scale, scale_ref.shape)

    def step(s, carry):
        for x in range(3):

            @pl.when(s < steps)
            def _():
                stage_wait(x)
                pl.when(s >= SENDS)(lambda: send_wait(s - SENDS, x))
                gather(s, x)
                with_arrival(s, x, send_start)
                pl.when(s + 1 < steps)(lambda: tp_start(s + 1, x))
                if x == 0:
                    pl.when(s == 0)(begin_total)
                if x == 2:
                    pl.when(s == 0)(spread_total)
                after, y = (s, x + 1) if x < 2 else (s + 1, 0)

                @pl.when(after < steps)
                def _():
                    tp_wait(after, y, tp_landed)
                    stage_start(after, y)

            @pl.when(s >= 1)
            def _():
                recv_wait(s - 1, x)
                with_arrival(s - 1, x, place)

        @pl.when(s >= 1)
        def _():
            pl.when(s == 1)(end_total)
            adam(s - 1)

        return carry

    lax.fori_loop(0, steps + 1, step, 0)
    for x in range(3):
        for s in range(max(0, steps - SENDS), steps):
            send_wait(s, x)
        over_steps(lambda s: tp_wait(s, x, tp_sent))
    partial_wait(0, 0)
    partial_wait(1, 0)


def drain_kernel(held, *refs):
    outs, sem = refs[:-1], refs[-1]
    copies = [
        pltpu.make_async_copy(
            held.at[i, u], out.at[:, u * LANES : (u + 1) * LANES], sem.at[i, u]
        )
        for i, out in enumerate(outs)
        for u in range(held.shape[1])
    ]
    for copy in copies:
        copy.start()
    for copy in copies:
        copy.wait()


def per_device(entries, saved_master, saved_first, saved_second, grad, row_target, step):
    tp_count, fsdp_count = lax.axis_size("tp"), lax.axis_size("fsdp")
    block_index = lax.axis_index("fsdp")
    block_rows, columns = grad.shape
    piece = saved_master.shape[0]
    all_rows = row_target.shape[0]
    pair = block_rows // fsdp_count
    steps = columns // LANES

    mine = lax.dynamic_slice_in_dim(row_target, block_index * block_rows, block_rows)
    send_order = jnp.argsort(mine, stable=True).astype(jnp.int32)
    send_idx = send_order

    in_block = row_target // block_rows == block_index
    sort_keys = jnp.where(in_block, row_target, all_rows)
    source_block = jnp.argsort(sort_keys, stable=True)[:block_rows].astype(jnp.int32) // block_rows
    local = jnp.arange(block_rows, dtype=jnp.int32)
    before = (source_block[None, :] == source_block[:, None]) & (local[None, :] < local[:, None])
    place_idx = source_block * pair + jnp.sum(before.astype(jnp.int32), axis=1)

    taken = step[0].astype(jnp.float32)
    fixes = jnp.stack(
        [
            1.0 - jnp.power(jnp.float32(beta_one), taken),
            1.0 - jnp.power(jnp.float32(beta_two), taken),
        ]
    )

    def kernel(*refs):
        restore_kernel((tp_count, fsdp_count), entries, *refs)

    smem = pl.BlockSpec(memory_space=pltpu.SMEM)
    hbm = pl.BlockSpec(memory_space=pltpu.HBM)
    vmem = pl.BlockSpec(memory_space=pltpu.VMEM)
    dma = pltpu.SemaphoreType.DMA
    wide = jnp.float32
    blocks = (block_rows,) if pair % 8 == 0 else (fsdp_count, pair)
    arrival = pltpu.VMEM((*blocks, LANES), wide)
    held, _ = pl.pallas_call(
        kernel,
        out_shape=[
            pltpu.VMEM((4, steps, block_rows, LANES), wide),
            jax.ShapeDtypeStruct((steps, 3, tp_count, piece, LANES), wide),
        ],
        in_specs=[smem] * 3 + [hbm] * 4,
        out_specs=[vmem, hbm],
        scratch_shapes=[
            pltpu.VMEM((tp_count * piece, LANES), wide),
            pltpu.VMEM((tp_count * piece, LANES), wide),
            pltpu.VMEM((tp_count * piece, LANES), wide),
            pltpu.VMEM((SENDS, 3, fsdp_count, pair, LANES), wide),
        ]
        + [arrival] * (3 * ARRIVALS)
        + [
            pltpu.VMEM((steps, block_rows, LANES), grad.dtype),
            pltpu.VMEM((1, LANES), wide),
            pltpu.VMEM((1, LANES), wide),
            pltpu.VMEM((tp_count, 1, LANES), wide),
            pltpu.VMEM((fsdp_count, 1, LANES), wide),
            pltpu.VMEM((1, LANES), wide),
            dma((steps, 3)),
            dma((steps, 3)),
            dma((3,)),
            dma((SENDS, 3)),
            dma((steps, 3)),
            dma,
            dma((4,)),
        ],
        compiler_params=pltpu.CompilerParams(
            has_side_effects=True, vmem_limit_bytes=22 << 20
        ),
        name="restore",
    )(send_idx, place_idx, fixes, saved_master, saved_first, saved_second, grad)

    out = jax.ShapeDtypeStruct((block_rows, columns), wide)
    return tuple(
        pl.pallas_call(
            drain_kernel,
            out_shape=[out] * 4,
            in_specs=[pl.BlockSpec(memory_space=pl.ANY)],
            out_specs=[hbm] * 4,
            scratch_shapes=[dma((4, steps))],
            compiler_params=pltpu.CompilerParams(vmem_limit_bytes=1 << 20),
            name="drain",
        )(held)
    )


def solution(mesh):
    in_specs = (
        P(("fsdp", "tp"), None),
        P(("fsdp", "tp"), None),
        P(("fsdp", "tp"), None),
        P("fsdp", "tp"),
        P(),
        P(),
    )
    out_specs = (P("fsdp", "tp"), P("fsdp", "tp"), P("fsdp", "tp"), P("fsdp", "tp"))

    def whole(saved_master, saved_first, saved_second, grad, row_target, step):
        def body(*args):
            return per_device(grad.shape[0] * grad.shape[1], *args)

        return jax.shard_map(
            body, mesh=mesh, in_specs=in_specs, out_specs=out_specs, check_vma=False
        )(saved_master, saved_first, saved_second, grad, row_target, step)

    return whole
```

```python
import math

import jax
import jax.numpy as jnp
from jax import lax
from jax.experimental import pallas as pl
from jax.experimental.pallas import tpu as pltpu
from jax.sharding import PartitionSpec as P

beta_one = 0.9
beta_two = 0.95
epsilon = 1e-08
learn_rate = 0.001
weight_decay = 0.1

LANES = 128
SENDS = 2
ARRIVALS = 3
UNROLL = 32
MESH = pl.DeviceIdType.MESH


def partner_steps(count):
    bits = count.bit_length() - 1
    if 1 << bits != count:
        return list(range(1, count))
    return [int(format(i, f"0{bits}b")[::-1], 2) for i in range(1, count)]


def restore_kernel(count, entries, *refs):
    tp_count, fsdp_count = count
    step_ref, target_ref, master_ref, first_ref, second_ref, grad_ref = refs[:6]
    out, landed = refs[6:8]
    send_idx, place_idx, send_table, place_table, spread, table_sem = refs[8:14]
    stages, send = refs[14:17], refs[17]
    arrivals = [refs[18 + 3 * i : 21 + 3 * i] for i in range(ARRIVALS)]
    grad, partial, partial_row, from_tp, from_fsdp, scale_ref = refs[-13:-7]
    tp_sent, tp_landed, staged, sent, arrived, grad_sem, partial_sems = refs[-7:]
    f, t = lax.axis_index("fsdp"), lax.axis_index("tp")
    saved = (master_ref, first_ref, second_ref)
    steps, block_rows = out.shape[1], out.shape[2]
    columns = steps * LANES
    piece = master_ref.shape[0]
    pair = block_rows // fsdp_count
    power = fsdp_count & (fsdp_count - 1) == 0
    flat = pair % 8 == 0

    def along_tp(d):
        return lax.rem(t + d, tp_count)

    def along_fsdp(d):
        return jnp.bitwise_xor(f, d) if power else lax.rem(f + d, fsdp_count)

    def unit(ref, half, s):
        return ref.at[:, pl.ds(pl.multiple_of(half * columns + s * LANES, LANES), LANES)]

    def half_rows(half):
        return pl.ds(pl.multiple_of(half * piece, 8), piece)

    def tp_start(s, x, first=False):
        for d in range(1, tp_count):
            peer = along_tp(d)
            pltpu.make_async_remote_copy(
                src_ref=unit(saved[x], peer, s),
                dst_ref=stages[x].at[half_rows(t)] if first else landed.at[s, x, t],
                send_sem=tp_sent.at[s, x],
                recv_sem=tp_landed.at[s, x],
                device_id=(f, peer),
                device_id_type=MESH,
            ).start()

    def tp_wait(s, x, sem):
        if tp_count > 1:
            whole = landed.at[s, x, pl.ds(0, tp_count - 1)]
            pltpu.make_async_copy(whole, whole, sem.at[s, x]).wait()

    def stage_own(s, x):
        return pltpu.make_async_copy(unit(saved[x], t, s), stages[x].at[half_rows(t)], staged.at[x])

    def stage_start(s, x):
        stage_own(s, x).start()
        for d in range(1, tp_count):
            half = along_tp(d)
            source = landed.at[s, x, half]
            pltpu.make_async_copy(source, stages[x].at[half_rows(half)], staged.at[x]).start()

    def stage_wait(s, x):
        pl.when(s == 0)(lambda: (stage_own(s, x).wait(), tp_wait(s, x, tp_landed))[1])
        whole = stages[x]
        pl.when(s > 0)(lambda: pltpu.make_async_copy(whole, whole, staged.at[x]).wait())

    def with_arrival(s, x, body):
        for i, held in enumerate(arrivals):
            pl.when(lax.rem(s, ARRIVALS) == i)(lambda recv=held[x]: body(s, x, recv))

    def block_of(recv, b):
        return pl.ds(pl.multiple_of(b * pair, 8), pair) if flat else b

    def send_start(s, x, recv):
        slot = lax.rem(s, SENDS)
        recv[block_of(recv, f)] = send[slot, x, f]
        for d in partner_steps(fsdp_count):
            peer = along_fsdp(d)
            pltpu.make_async_remote_copy(
                src_ref=send.at[slot, x, peer],
                dst_ref=recv.at[block_of(recv, f)],
                send_sem=sent.at[slot, x],
                recv_sem=arrived.at[s, x],
                device_id=(peer, t),
                device_id_type=MESH,
            ).start()

    def exchanged():
        return send.at[0, 0, pl.ds(0, fsdp_count - 1)]

    def send_wait(s, x):
        pltpu.make_async_copy(exchanged(), exchanged(), sent.at[lax.rem(s, SENDS), x]).wait()

    def recv_wait(s, x):
        pltpu.make_async_copy(exchanged(), exchanged(), arrived.at[s, x]).wait()

    lines = block_rows // LANES
    square = (LANES, LANES)
    lane = lax.broadcasted_iota(jnp.int32, square, 1)
    sublane = lax.broadcasted_iota(jnp.int32, square, 0)

    def across(column):
        return jnp.broadcast_to(column, square)

    def turned(row):
        return jnp.transpose(across(row))

    def ones_where(mask):
        return jnp.where(mask, 1, 0)

    def inside(index):
        return jnp.clip(index, 0, block_rows - 1)

    def to_scalars(table, idx):
        copy = pltpu.make_async_copy(table, idx, table_sem)
        copy.start()
        copy.wait()

    def fill_send_idx():
        mine = [target_ref[pl.ds(f * lines + c, 1), :] for c in range(lines)]
        for c in range(lines):
            column, smaller = turned(mine[c]), jnp.zeros(square, jnp.int32)
            for row in mine:
                smaller = smaller + ones_where(row < column)
            spread[c] = across(jnp.sum(smaller, axis=1, keepdims=True))
        for c in range(lines):
            source = jnp.zeros(square, jnp.int32)
            for d in range(lines):
                source = source + jnp.where(spread[d] == c * LANES + lane, d * LANES + sublane, 0)
            send_table[pl.ds(c, 1), :] = inside(jnp.sum(source, axis=0, keepdims=True))
        to_scalars(send_table, send_idx)

    def fill_place_idx():
        def one_line(c, carry):
            wanted = f * block_rows + c * LANES + sublane

            def one_row(k, block):
                return block + jnp.where(target_ref[pl.ds(k, 1), :] == wanted, k // lines, 0)

            block = lax.fori_loop(
                0, target_ref.shape[0], one_row, jnp.zeros(square, jnp.int32), unroll=4
            )
            spread[c] = across(jnp.sum(block, axis=1, keepdims=True))
            place_table[pl.ds(c, 1), :] = jnp.transpose(spread[c])[:1]
            return carry

        lax.fori_loop(0, lines, one_line, 0)
        blocks = [place_table[pl.ds(c, 1), :] for c in range(lines)]
        for c in range(lines):
            column = spread[c]
            earlier = ones_where((blocks[c] == column) & (lane < sublane))
            for d in range(c):
                earlier = earlier + ones_where(blocks[d] == column)
            rank = jnp.sum(earlier, axis=1, keepdims=True)
            place_table[pl.ds(c, 1), :] = inside(jnp.transpose(column * pair + across(rank))[:1])
        to_scalars(place_table, place_idx)

    def power_of(base):
        def one_bit(i, carry):
            result, factor = carry
            odd = lax.shift_right_logical(step_ref[0], i) & 1
            return jnp.where(odd == 1, result * factor, result), factor * factor

        return lax.fori_loop(0, 31, one_bit, (jnp.float32(1.0), jnp.float32(base)))[0]

    run = math.gcd(pair, UNROLL)

    def gather(s, x):
        slot = lax.rem(s, SENDS)

        def one_block(b, carry):
            def one_run(k, carry):
                at = b * pair + k * run
                line, column = at // LANES, at % LANES
                for u in range(run):
                    row = send_idx[line, column + u]
                    send[slot, x, b, pl.ds(k * run + u, 1), :] = stages[x][pl.ds(row, 1), :]
                return carry

            return lax.fori_loop(0, pair // run, one_run, carry)

        lax.fori_loop(0, fsdp_count, one_block, 0)

    def place(s, x, recv):
        def one_line(c, carry):
            def one_run(k, carry):
                for u in range(UNROLL):
                    index = place_idx[c, k * UNROLL + u]
                    if flat:
                        row = recv[pl.ds(index, 1), :]
                    else:
                        row = recv[index // pair, pl.ds(index % pair, 1), :]
                    out[x, s, pl.ds(c * LANES + k * UNROLL + u, 1), :] = row
                return carry

            return lax.fori_loop(0, LANES // UNROLL, one_run, carry)

        lax.fori_loop(0, lines, one_line, 0)

    tile = math.gcd(block_rows, 64)

    def adam(s):
        scale = scale_ref[...]
        first_fix = 1.0 - power_of(beta_one)
        second_fix = 1.0 - power_of(beta_two)

        def one_tile(k, carry):
            rows = pl.ds(pl.multiple_of(k * tile, tile), tile)
            clipped = scale * grad[s, rows, :].astype(jnp.float32)
            master = out[0, s, rows, :]
            first_new = beta_one * out[1, s, rows, :] + (1.0 - beta_one) * clipped
            second_new = beta_two * out[2, s, rows, :] + (1.0 - beta_two) * clipped * clipped
            first_hat = first_new / first_fix
            second_hat = second_new / second_fix
            direction = first_hat / (jnp.sqrt(second_hat) + epsilon) + weight_decay * master
            out[0, s, rows, :] = master - learn_rate * direction
            out[1, s, rows, :] = first_new
            out[2, s, rows, :] = second_new
            out[3, s, rows, :] = direction
            return carry

        lax.fori_loop(0, block_rows // tile, one_tile, 0)

    def square_sum():
        def one_unit(s, total):
            def one_tile(k, total):
                rows = pl.ds(pl.multiple_of(k * tile, tile), tile)
                wide = grad[s, rows, :].astype(jnp.float32)
                return total + wide * wide

            return lax.fori_loop(0, block_rows // tile, one_tile, total)

        total = lax.fori_loop(0, steps, one_unit, jnp.zeros((tile, LANES), jnp.float32))
        return jnp.sum(total, axis=0, keepdims=True)

    def partial_copies(which):
        if which == 0:
            peers = [(f, along_tp(d)) for d in range(1, tp_count)]
            source, target = partial, from_tp.at[t]
        else:
            peers = [(along_fsdp(d), t) for d in partner_steps(fsdp_count)]
            source, target = partial_row, from_fsdp.at[f]
        return [
            pltpu.make_async_remote_copy(
                src_ref=source,
                dst_ref=target,
                send_sem=partial_sems.at[2 * which],
                recv_sem=partial_sems.at[2 * which + 1],
                device_id=peer,
                device_id_type=MESH,
            )
            for peer in peers
        ]

    def partial_wait(which, side):
        held = (from_tp, from_fsdp)[which]
        members = (tp_count, fsdp_count)[which]
        if members > 1:
            whole = held.at[pl.ds(0, members - 1)]
            pltpu.make_async_copy(whole, whole, partial_sems.at[2 * which + side]).wait()

    def summed(held, members):
        total = held[0]
        for i in range(1, members):
            total = total + held[i]
        return total

    def grad_copy(s):
        return pltpu.make_async_copy(unit(grad_ref, 0, s), grad.at[s], grad_sem)

    def over_steps(body):
        lax.fori_loop(0, steps, lambda s, carry: (body(s), carry)[1], 0)

    for x in range(3):
        tp_start(0, x, True)
        stage_own(0, x).start()
    over_steps(lambda s: grad_copy(s).start())
    fill_send_idx()

    def begin_total():
        pltpu.make_async_copy(grad, grad, grad_sem).wait()
        own = square_sum()
        partial[...] = own
        from_tp[t] = own
        for copy in partial_copies(0):
            copy.start()

    def spread_total():
        partial_wait(0, 1)
        row = summed(from_tp, tp_count)
        partial_row[...] = row
        from_fsdp[f] = row
        for copy in partial_copies(1):
            copy.start()

    def end_total():
        partial_wait(1, 1)
        total = jnp.sum(summed(from_fsdp, fsdp_count), axis=1, keepdims=True)
        scale = jnp.minimum(1.0, math.sqrt(entries) / jnp.sqrt(total))
        scale_ref[...] = jnp.broadcast_to(scale, scale_ref.shape)

    def step(s, carry):
        for x in range(3):

            @pl.when(s < steps)
            def _():
                stage_wait(s, x)
                pl.when(s >= SENDS)(lambda: send_wait(s - SENDS, x))
                gather(s, x)
                with_arrival(s, x, send_start)
                pl.when(s + 1 < steps)(lambda: tp_start(s + 1, x))
                if x == 0:
                    pl.when(s == 0)(begin_total)
                if x == 1:
                    pl.when(s == 0)(fill_place_idx)
                if x == 2:
                    pl.when(s == 0)(spread_total)
                after, y = (s, x + 1) if x < 2 else (s + 1, 0)

                @pl.when((after > 0) & (after < steps))
                def _():
                    tp_wait(after, y, tp_landed)
                    stage_start(after, y)

            @pl.when(s >= 1)
            def _():
                recv_wait(s - 1, x)
                with_arrival(s - 1, x, place)

        @pl.when(s >= 1)
        def _():
            pl.when(s == 1)(end_total)
            adam(s - 1)

        return carry

    lax.fori_loop(0, steps + 1, step, 0)
    for x in range(3):
        for s in range(max(0, steps - SENDS), steps):
            send_wait(s, x)
        over_steps(lambda s: tp_wait(s, x, tp_sent))
    partial_wait(0, 0)
    partial_wait(1, 0)


def drain_kernel(held, *refs):
    outs, sem = refs[:-1], refs[-1]
    copies = [
        pltpu.make_async_copy(
            held.at[i, u], out.at[:, u * LANES : (u + 1) * LANES], sem.at[i, u]
        )
        for i, out in enumerate(outs)
        for u in range(held.shape[1])
    ]
    for copy in copies:
        copy.start()
    for copy in copies:
        copy.wait()


def per_device(entries, saved_master, saved_first, saved_second, grad, row_target, step):
    tp_count, fsdp_count = lax.axis_size("tp"), lax.axis_size("fsdp")
    block_rows, columns = grad.shape
    piece = saved_master.shape[0]
    lines = block_rows // LANES
    pair = block_rows // fsdp_count
    steps = columns // LANES

    def kernel(*refs):
        restore_kernel((tp_count, fsdp_count), entries, *refs)

    smem = pl.BlockSpec(memory_space=pltpu.SMEM)
    hbm = pl.BlockSpec(memory_space=pltpu.HBM)
    vmem = pl.BlockSpec(memory_space=pltpu.VMEM)
    dma = pltpu.SemaphoreType.DMA
    wide = jnp.float32
    blocks = (block_rows,) if pair % 8 == 0 else (fsdp_count, pair)
    arrival = pltpu.VMEM((*blocks, LANES), wide)
    held, _ = pl.pallas_call(
        kernel,
        out_shape=[
            pltpu.VMEM((4, steps, block_rows, LANES), wide),
            jax.ShapeDtypeStruct((steps, 3, tp_count, piece, LANES), wide),
        ],
        in_specs=[smem, vmem] + [hbm] * 4,
        out_specs=[vmem, hbm],
        scratch_shapes=[
            pltpu.SMEM((lines, LANES), jnp.int32),
            pltpu.SMEM((lines, LANES), jnp.int32),
            pltpu.VMEM((lines, LANES), jnp.int32),
            pltpu.VMEM((lines, LANES), jnp.int32),
            pltpu.VMEM((lines, LANES, LANES), jnp.int32),
            dma,
            pltpu.VMEM((tp_count * piece, LANES), wide),
            pltpu.VMEM((tp_count * piece, LANES), wide),
            pltpu.VMEM((tp_count * piece, LANES), wide),
            pltpu.VMEM((SENDS, 3, fsdp_count, pair, LANES), wide),
        ]
        + [arrival] * (3 * ARRIVALS)
        + [
            pltpu.VMEM((steps, block_rows, LANES), grad.dtype),
            pltpu.VMEM((1, LANES), wide),
            pltpu.VMEM((1, LANES), wide),
            pltpu.VMEM((tp_count, 1, LANES), wide),
            pltpu.VMEM((fsdp_count, 1, LANES), wide),
            pltpu.VMEM((1, LANES), wide),
            dma((steps, 3)),
            dma((steps, 3)),
            dma((3,)),
            dma((SENDS, 3)),
            dma((steps, 3)),
            dma,
            dma((4,)),
        ],
        compiler_params=pltpu.CompilerParams(
            has_side_effects=True, vmem_limit_bytes=22 << 20
        ),
        name="restore",
    )(step, row_target.reshape(-1, LANES), saved_master, saved_first, saved_second, grad)

    out = jax.ShapeDtypeStruct((block_rows, columns), wide)
    return tuple(
        pl.pallas_call(
            drain_kernel,
            out_shape=[out] * 4,
            in_specs=[pl.BlockSpec(memory_space=pl.ANY)],
            out_specs=[hbm] * 4,
            scratch_shapes=[dma((4, steps))],
            compiler_params=pltpu.CompilerParams(vmem_limit_bytes=1 << 20),
            name="drain",
        )(held)
    )


def solution(mesh):
    in_specs = (
        P(("fsdp", "tp"), None),
        P(("fsdp", "tp"), None),
        P(("fsdp", "tp"), None),
        P("fsdp", "tp"),
        P(),
        P(),
    )
    out_specs = (P("fsdp", "tp"), P("fsdp", "tp"), P("fsdp", "tp"), P("fsdp", "tp"))

    def whole(saved_master, saved_first, saved_second, grad, row_target, step):
        def body(*args):
            return per_device(grad.shape[0] * grad.shape[1], *args)

        return jax.shard_map(
            body, mesh=mesh, in_specs=in_specs, out_specs=out_specs, check_vma=False
        )(saved_master, saved_first, saved_second, grad, row_target, step)

    return whole
```

```python
import math

import jax
import jax.numpy as jnp
from jax import lax
from jax.experimental import pallas as pl
from jax.experimental.pallas import tpu as pltpu
from jax.sharding import PartitionSpec as P

beta_one = 0.9
beta_two = 0.95
epsilon = 1e-08
learn_rate = 0.001
weight_decay = 0.1

LANES = 128
SENDS = 2
ARRIVALS = 3
UNROLL = 32
MESH = pl.DeviceIdType.MESH


def partner_steps(count):
    bits = count.bit_length() - 1
    if 1 << bits != count:
        return list(range(1, count))
    return [int(format(i, f"0{bits}b")[::-1], 2) for i in range(1, count)]


def restore_kernel(count, entries, *refs):
    tp_count, fsdp_count = count
    step_ref, target_ref, master_ref, first_ref, second_ref, grad_ref = refs[:6]
    out, landed = refs[6:8]
    send_idx, place_idx, send_table, place_table, spread, table_sem = refs[8:14]
    stages, send = refs[14:17], refs[17]
    arrivals = [refs[18 + 3 * i : 21 + 3 * i] for i in range(ARRIVALS)]
    grad, partial, partial_row, from_tp, from_fsdp, scale_ref = refs[-13:-7]
    tp_sent, tp_landed, staged, sent, arrived, grad_sem, partial_sems = refs[-7:]
    f, t = lax.axis_index("fsdp"), lax.axis_index("tp")
    saved = (master_ref, first_ref, second_ref)
    steps, block_rows = out.shape[1], out.shape[2]
    columns = steps * LANES
    piece = master_ref.shape[0]
    pair = block_rows // fsdp_count
    power = fsdp_count & (fsdp_count - 1) == 0
    flat = pair % 8 == 0

    def along_tp(d):
        return lax.rem(t + d, tp_count)

    def along_fsdp(d):
        return jnp.bitwise_xor(f, d) if power else lax.rem(f + d, fsdp_count)

    def unit(ref, half, s):
        return ref.at[:, pl.ds(pl.multiple_of(half * columns + s * LANES, LANES), LANES)]

    def half_rows(half):
        return pl.ds(pl.multiple_of(half * piece, 8), piece)

    def tp_start(s, x, first=False):
        for d in range(1, tp_count):
            peer = along_tp(d)
            pltpu.make_async_remote_copy(
                src_ref=unit(saved[x], peer, s),
                dst_ref=stages[x].at[half_rows(t)] if first else landed.at[s, x, t],
                send_sem=tp_sent.at[s, x],
                recv_sem=tp_landed.at[s, x],
                device_id=(f, peer),
                device_id_type=MESH,
            ).start()

    def tp_wait(s, x, sem):
        if tp_count > 1:
            whole = landed.at[s, x, pl.ds(0, tp_count - 1)]
            pltpu.make_async_copy(whole, whole, sem.at[s, x]).wait()

    def stage_own(s, x):
        return pltpu.make_async_copy(unit(saved[x], t, s), stages[x].at[half_rows(t)], staged.at[x])

    def stage_start(s, x):
        stage_own(s, x).start()
        for d in range(1, tp_count):
            half = along_tp(d)
            source = landed.at[s, x, half]
            pltpu.make_async_copy(source, stages[x].at[half_rows(half)], staged.at[x]).start()

    def stage_wait(s, x):
        pl.when(s == 0)(lambda: (stage_own(s, x).wait(), tp_wait(s, x, tp_landed))[1])
        whole = stages[x]
        pl.when(s > 0)(lambda: pltpu.make_async_copy(whole, whole, staged.at[x]).wait())

    def with_arrival(s, x, body):
        for i, held in enumerate(arrivals):
            pl.when(lax.rem(s, ARRIVALS) == i)(lambda recv=held[x]: body(s, x, recv))

    def block_of(recv, b):
        return pl.ds(pl.multiple_of(b * pair, 8), pair) if flat else b

    def send_start(s, x, recv):
        slot = lax.rem(s, SENDS)
        recv[block_of(recv, f)] = send[slot, x, f]
        for d in partner_steps(fsdp_count):
            peer = along_fsdp(d)
            pltpu.make_async_remote_copy(
                src_ref=send.at[slot, x, peer],
                dst_ref=recv.at[block_of(recv, f)],
                send_sem=sent.at[slot, x],
                recv_sem=arrived.at[s, x],
                device_id=(peer, t),
                device_id_type=MESH,
            ).start()

    def exchanged():
        return send.at[0, 0, pl.ds(0, fsdp_count - 1)]

    def send_wait(s, x):
        pltpu.make_async_copy(exchanged(), exchanged(), sent.at[lax.rem(s, SENDS), x]).wait()

    def recv_wait(s, x):
        pltpu.make_async_copy(exchanged(), exchanged(), arrived.at[s, x]).wait()

    lines = block_rows // LANES
    square = (LANES, LANES)
    lane = lax.broadcasted_iota(jnp.int32, square, 1)
    sublane = lax.broadcasted_iota(jnp.int32, square, 0)

    def across(column):
        return jnp.broadcast_to(column, square)

    def turned(row):
        return jnp.transpose(across(row))

    def ones_where(mask):
        return jnp.where(mask, 1, 0)

    def inside(index):
        return jnp.clip(index, 0, block_rows - 1)

    def to_scalars(table, idx):
        copy = pltpu.make_async_copy(table, idx, table_sem)
        copy.start()
        copy.wait()

    def fill_send_idx():
        mine = [target_ref[pl.ds(f * lines + c, 1), :] for c in range(lines)]
        for c in range(lines):
            column, smaller = turned(mine[c]), jnp.zeros(square, jnp.int32)
            for row in mine:
                smaller = smaller + ones_where(row < column)
            spread[c] = across(jnp.sum(smaller, axis=1, keepdims=True))
        for c in range(lines):
            source = jnp.zeros(square, jnp.int32)
            for d in range(lines):
                source = source + jnp.where(spread[d] == c * LANES + lane, d * LANES + sublane, 0)
            send_table[pl.ds(c, 1), :] = inside(jnp.sum(source, axis=0, keepdims=True))
        to_scalars(send_table, send_idx)

    def fill_place_idx():
        def one_line(c, carry):
            wanted = f * block_rows + c * LANES + sublane

            def one_row(k, block):
                return block + jnp.where(target_ref[pl.ds(k, 1), :] == wanted, k // lines, 0)

            block = lax.fori_loop(
                0, target_ref.shape[0], one_row, jnp.zeros(square, jnp.int32), unroll=4
            )
            spread[c] = across(jnp.sum(block, axis=1, keepdims=True))
            place_table[pl.ds(c, 1), :] = jnp.transpose(spread[c])[:1]
            return carry

        lax.fori_loop(0, lines, one_line, 0)
        blocks = [place_table[pl.ds(c, 1), :] for c in range(lines)]
        for c in range(lines):
            column = spread[c]
            earlier = ones_where((blocks[c] == column) & (lane < sublane))
            for d in range(c):
                earlier = earlier + ones_where(blocks[d] == column)
            rank = jnp.sum(earlier, axis=1, keepdims=True)
            place_table[pl.ds(c, 1), :] = inside(jnp.transpose(column * pair + across(rank))[:1])
        to_scalars(place_table, place_idx)

    def power_of(base):
        def one_bit(i, carry):
            result, factor = carry
            odd = lax.shift_right_logical(step_ref[0], i) & 1
            return jnp.where(odd == 1, result * factor, result), factor * factor

        return lax.fori_loop(0, 31, one_bit, (jnp.float32(1.0), jnp.float32(base)))[0]

    run = math.gcd(pair, UNROLL)

    def gather(s, x):
        slot = lax.rem(s, SENDS)

        def one_block(b, carry):
            def one_run(k, carry):
                at = b * pair + k * run
                line, column = at // LANES, at % LANES
                for u in range(run):
                    row = send_idx[line, column + u]
                    send[slot, x, b, pl.ds(k * run + u, 1), :] = stages[x][pl.ds(row, 1), :]
                return carry

            return lax.fori_loop(0, pair // run, one_run, carry)

        lax.fori_loop(0, fsdp_count, one_block, 0)

    def place(s, x, recv):
        def one_line(c, carry):
            def one_run(k, carry):
                for u in range(UNROLL):
                    index = place_idx[c, k * UNROLL + u]
                    if flat:
                        row = recv[pl.ds(index, 1), :]
                    else:
                        row = recv[index // pair, pl.ds(index % pair, 1), :]
                    out[x, s, pl.ds(c * LANES + k * UNROLL + u, 1), :] = row
                return carry

            return lax.fori_loop(0, LANES // UNROLL, one_run, carry)

        lax.fori_loop(0, lines, one_line, 0)

    tile = math.gcd(block_rows, 64)

    def adam(s):
        scale = scale_ref[...]
        first_fix = 1.0 - power_of(beta_one)
        second_fix = 1.0 - power_of(beta_two)

        def one_tile(k, carry):
            rows = pl.ds(pl.multiple_of(k * tile, tile), tile)
            clipped = scale * grad[s, rows, :].astype(jnp.float32)
            master = out[0, s, rows, :]
            first_new = beta_one * out[1, s, rows, :] + (1.0 - beta_one) * clipped
            second_new = beta_two * out[2, s, rows, :] + (1.0 - beta_two) * clipped * clipped
            first_hat = first_new / first_fix
            second_hat = second_new / second_fix
            direction = first_hat / (jnp.sqrt(second_hat) + epsilon) + weight_decay * master
            out[0, s, rows, :] = master - learn_rate * direction
            out[1, s, rows, :] = first_new
            out[2, s, rows, :] = second_new
            out[3, s, rows, :] = direction
            return carry

        lax.fori_loop(0, block_rows // tile, one_tile, 0)

    def square_sum():
        def one_unit(s, total):
            def one_tile(k, total):
                rows = pl.ds(pl.multiple_of(k * tile, tile), tile)
                wide = grad[s, rows, :].astype(jnp.float32)
                return total + wide * wide

            return lax.fori_loop(0, block_rows // tile, one_tile, total)

        total = lax.fori_loop(0, steps, one_unit, jnp.zeros((tile, LANES), jnp.float32))
        return jnp.sum(total, axis=0, keepdims=True)

    def partial_copies(which):
        if which == 0:
            peers = [(f, along_tp(d)) for d in range(1, tp_count)]
            source, target = partial, from_tp.at[t]
        else:
            peers = [(along_fsdp(d), t) for d in partner_steps(fsdp_count)]
            source, target = partial_row, from_fsdp.at[f]
        return [
            pltpu.make_async_remote_copy(
                src_ref=source,
                dst_ref=target,
                send_sem=partial_sems.at[2 * which],
                recv_sem=partial_sems.at[2 * which + 1],
                device_id=peer,
                device_id_type=MESH,
            )
            for peer in peers
        ]

    def partial_wait(which, side):
        held = (from_tp, from_fsdp)[which]
        members = (tp_count, fsdp_count)[which]
        if members > 1:
            whole = held.at[pl.ds(0, members - 1)]
            pltpu.make_async_copy(whole, whole, partial_sems.at[2 * which + side]).wait()

    def summed(held, members):
        total = held[0]
        for i in range(1, members):
            total = total + held[i]
        return total

    def grad_copy(s):
        return pltpu.make_async_copy(unit(grad_ref, 0, s), grad.at[s], grad_sem)

    def over_steps(body):
        lax.fori_loop(0, steps, lambda s, carry: (body(s), carry)[1], 0)

    barrier = pltpu.get_barrier_semaphore()
    partners = [(along_fsdp(d), t) for d in partner_steps(fsdp_count)]
    partners += [(f, along_tp(d)) for d in range(1, tp_count)]
    for peer in partners:
        pl.semaphore_signal(barrier, inc=1, device_id=peer, device_id_type=MESH)
    for x in range(3):
        stage_own(0, x).start()
    pl.semaphore_wait(barrier, len(partners))
    for x in range(3):
        tp_start(0, x, True)
    over_steps(lambda s: grad_copy(s).start())
    fill_send_idx()

    def begin_total():
        pltpu.make_async_copy(grad, grad, grad_sem).wait()
        own = square_sum()
        partial[...] = own
        from_tp[t] = own
        for copy in partial_copies(0):
            copy.start()

    def spread_total():
        partial_wait(0, 1)
        row = summed(from_tp, tp_count)
        partial_row[...] = row
        from_fsdp[f] = row
        for copy in partial_copies(1):
            copy.start()

    def end_total():
        partial_wait(1, 1)
        total = jnp.sum(summed(from_fsdp, fsdp_count), axis=1, keepdims=True)
        scale = jnp.minimum(1.0, math.sqrt(entries) / jnp.sqrt(total))
        scale_ref[...] = jnp.broadcast_to(scale, scale_ref.shape)

    def step(s, carry):
        for x in range(3):

            @pl.when(s < steps)
            def _():
                stage_wait(s, x)
                pl.when(s >= SENDS)(lambda: send_wait(s - SENDS, x))
                gather(s, x)
                with_arrival(s, x, send_start)
                pl.when(s + 1 < steps)(lambda: tp_start(s + 1, x))
                if x == 0:
                    pl.when(s == 0)(begin_total)
                if x == 1:
                    pl.when(s == 0)(fill_place_idx)
                if x == 2:
                    pl.when(s == 0)(spread_total)
                after, y = (s, x + 1) if x < 2 else (s + 1, 0)

                @pl.when((after > 0) & (after < steps))
                def _():
                    tp_wait(after, y, tp_landed)
                    stage_start(after, y)

            @pl.when(s >= 1)
            def _():
                recv_wait(s - 1, x)
                with_arrival(s - 1, x, place)

        @pl.when(s >= 1)
        def _():
            pl.when(s == 1)(end_total)
            adam(s - 1)

        return carry

    lax.fori_loop(0, steps + 1, step, 0)
    for x in range(3):
        for s in range(max(0, steps - SENDS), steps):
            send_wait(s, x)
        over_steps(lambda s: tp_wait(s, x, tp_sent))
    partial_wait(0, 0)
    partial_wait(1, 0)


def drain_kernel(held, *refs):
    outs, sem = refs[:-1], refs[-1]
    copies = [
        pltpu.make_async_copy(
            held.at[i, u], out.at[:, u * LANES : (u + 1) * LANES], sem.at[i, u]
        )
        for i, out in enumerate(outs)
        for u in range(held.shape[1])
    ]
    for copy in copies:
        copy.start()
    for copy in copies:
        copy.wait()


def per_device(entries, saved_master, saved_first, saved_second, grad, row_target, step):
    tp_count, fsdp_count = lax.axis_size("tp"), lax.axis_size("fsdp")
    block_rows, columns = grad.shape
    piece = saved_master.shape[0]
    lines = block_rows // LANES
    pair = block_rows // fsdp_count
    steps = columns // LANES

    def kernel(*refs):
        restore_kernel((tp_count, fsdp_count), entries, *refs)

    smem = pl.BlockSpec(memory_space=pltpu.SMEM)
    hbm = pl.BlockSpec(memory_space=pltpu.HBM)
    vmem = pl.BlockSpec(memory_space=pltpu.VMEM)
    dma = pltpu.SemaphoreType.DMA
    wide = jnp.float32
    blocks = (block_rows,) if pair % 8 == 0 else (fsdp_count, pair)
    arrival = pltpu.VMEM((*blocks, LANES), wide)
    held, _ = pl.pallas_call(
        kernel,
        out_shape=[
            pltpu.VMEM((4, steps, block_rows, LANES), wide),
            jax.ShapeDtypeStruct((steps, 3, tp_count, piece, LANES), wide),
        ],
        in_specs=[smem, vmem] + [hbm] * 4,
        out_specs=[vmem, hbm],
        scratch_shapes=[
            pltpu.SMEM((lines, LANES), jnp.int32),
            pltpu.SMEM((lines, LANES), jnp.int32),
            pltpu.VMEM((lines, LANES), jnp.int32),
            pltpu.VMEM((lines, LANES), jnp.int32),
            pltpu.VMEM((lines, LANES, LANES), jnp.int32),
            dma,
            pltpu.VMEM((tp_count * piece, LANES), wide),
            pltpu.VMEM((tp_count * piece, LANES), wide),
            pltpu.VMEM((tp_count * piece, LANES), wide),
            pltpu.VMEM((SENDS, 3, fsdp_count, pair, LANES), wide),
        ]
        + [arrival] * (3 * ARRIVALS)
        + [
            pltpu.VMEM((steps, block_rows, LANES), grad.dtype),
            pltpu.VMEM((1, LANES), wide),
            pltpu.VMEM((1, LANES), wide),
            pltpu.VMEM((tp_count, 1, LANES), wide),
            pltpu.VMEM((fsdp_count, 1, LANES), wide),
            pltpu.VMEM((1, LANES), wide),
            dma((steps, 3)),
            dma((steps, 3)),
            dma((3,)),
            dma((SENDS, 3)),
            dma((steps, 3)),
            dma,
            dma((4,)),
        ],
        compiler_params=pltpu.CompilerParams(
            has_side_effects=True, collective_id=0, vmem_limit_bytes=22 << 20
        ),
        name="restore",
    )(step, row_target.reshape(-1, LANES), saved_master, saved_first, saved_second, grad)

    out = jax.ShapeDtypeStruct((block_rows, columns), wide)
    return tuple(
        pl.pallas_call(
            drain_kernel,
            out_shape=[out] * 4,
            in_specs=[pl.BlockSpec(memory_space=pl.ANY)],
            out_specs=[hbm] * 4,
            scratch_shapes=[dma((4, steps))],
            compiler_params=pltpu.CompilerParams(vmem_limit_bytes=1 << 20),
            name="drain",
        )(held)
    )


def solution(mesh):
    in_specs = (
        P(("fsdp", "tp"), None),
        P(("fsdp", "tp"), None),
        P(("fsdp", "tp"), None),
        P("fsdp", "tp"),
        P(),
        P(),
    )
    out_specs = (P("fsdp", "tp"), P("fsdp", "tp"), P("fsdp", "tp"), P("fsdp", "tp"))

    def whole(saved_master, saved_first, saved_second, grad, row_target, step):
        def body(*args):
            return per_device(grad.shape[0] * grad.shape[1], *args)

        return jax.shard_map(
            body, mesh=mesh, in_specs=in_specs, out_specs=out_specs, check_vma=False
        )(saved_master, saved_first, saved_second, grad, row_target, step)

    return whole
```

```python
import math

import jax
import jax.numpy as jnp
from jax import lax
from jax.experimental import pallas as pl
from jax.experimental.pallas import tpu as pltpu
from jax.sharding import PartitionSpec as P

beta_one = 0.9
beta_two = 0.95
epsilon = 1e-08
learn_rate = 0.001
weight_decay = 0.1

LANES = 128
SENDS = 2
ARRIVALS = 3
UNROLL = 32
MESH = pl.DeviceIdType.MESH


def partner_steps(count):
    bits = count.bit_length() - 1
    if 1 << bits != count:
        return list(range(1, count))
    return [int(format(i, f"0{bits}b")[::-1], 2) for i in range(1, count)]


def power_of(base, step_ref):
    def one_bit(i, carry):
        result, factor = carry
        odd = lax.shift_right_logical(step_ref[0], i) & 1
        return jnp.where(odd == 1, result * factor, result), factor * factor

    return lax.fori_loop(0, 31, one_bit, (jnp.float32(1.0), jnp.float32(base)))[0]


def adam_unit(clipped_of, step_ref, state, result):
    first_fix = 1.0 - power_of(beta_one, step_ref)
    second_fix = 1.0 - power_of(beta_two, step_ref)
    tile = math.gcd(result.shape[1], 64)

    def one_tile(k, carry):
        rows = pl.ds(pl.multiple_of(k * tile, tile), tile)
        clipped = clipped_of(rows)
        master = state[0, rows, :]
        first_new = beta_one * state[1, rows, :] + (1.0 - beta_one) * clipped
        second_new = beta_two * state[2, rows, :] + (1.0 - beta_two) * clipped * clipped
        first_hat = first_new / first_fix
        second_hat = second_new / second_fix
        direction = first_hat / (jnp.sqrt(second_hat) + epsilon) + weight_decay * master
        result[0, rows, :] = master - learn_rate * direction
        result[1, rows, :] = first_new
        result[2, rows, :] = second_new
        result[3, rows, :] = direction
        return carry

    lax.fori_loop(0, result.shape[1] // tile, one_tile, 0)


def restore_kernel(count, entries, *refs):
    tp_count, fsdp_count = count
    step_ref, target_ref, master_ref, first_ref, second_ref, grad_ref = refs[:6]
    out, landed = refs[6:8]
    send_idx, place_idx, send_table, place_table, spread, table_sem = refs[8:14]
    stages, send = refs[14:17], refs[17]
    arrivals = [refs[18 + 3 * i : 21 + 3 * i] for i in range(ARRIVALS)]
    grad, partial, partial_row, from_tp, from_fsdp, scale_ref = refs[-13:-7]
    tp_sent, tp_landed, staged, sent, arrived, grad_sem, partial_sems = refs[-7:]
    f, t = lax.axis_index("fsdp"), lax.axis_index("tp")
    saved = (master_ref, first_ref, second_ref)
    steps, block_rows = out.shape[1], out.shape[2]
    columns = steps * LANES
    piece = master_ref.shape[0]
    pair = block_rows // fsdp_count
    power = fsdp_count & (fsdp_count - 1) == 0
    flat = pair % 8 == 0

    def along_tp(d):
        return lax.rem(t + d, tp_count)

    def along_fsdp(d):
        return jnp.bitwise_xor(f, d) if power else lax.rem(f + d, fsdp_count)

    def unit(ref, half, s):
        return ref.at[:, pl.ds(pl.multiple_of(half * columns + s * LANES, LANES), LANES)]

    def half_rows(half):
        return pl.ds(pl.multiple_of(half * piece, 8), piece)

    def tp_start(s, x, first=False):
        for d in range(1, tp_count):
            peer = along_tp(d)
            pltpu.make_async_remote_copy(
                src_ref=unit(saved[x], peer, s),
                dst_ref=stages[x].at[half_rows(t)] if first else landed.at[s, x, t],
                send_sem=tp_sent.at[s, x],
                recv_sem=tp_landed.at[s, x],
                device_id=(f, peer),
                device_id_type=MESH,
            ).start()

    def tp_wait(s, x, sem):
        if tp_count > 1:
            whole = landed.at[s, x, pl.ds(0, tp_count - 1)]
            pltpu.make_async_copy(whole, whole, sem.at[s, x]).wait()

    def stage_own(s, x):
        return pltpu.make_async_copy(unit(saved[x], t, s), stages[x].at[half_rows(t)], staged.at[x])

    def stage_start(s, x):
        stage_own(s, x).start()
        for d in range(1, tp_count):
            half = along_tp(d)
            source = landed.at[s, x, half]
            pltpu.make_async_copy(source, stages[x].at[half_rows(half)], staged.at[x]).start()

    def stage_wait(s, x):
        pl.when(s == 0)(lambda: (stage_own(s, x).wait(), tp_wait(s, x, tp_landed))[1])
        whole = stages[x]
        pl.when(s > 0)(lambda: pltpu.make_async_copy(whole, whole, staged.at[x]).wait())

    def with_arrival(s, x, body):
        for i, held in enumerate(arrivals):
            pl.when(lax.rem(s, ARRIVALS) == i)(lambda recv=held[x]: body(s, x, recv))

    def block_of(recv, b):
        return pl.ds(pl.multiple_of(b * pair, 8), pair) if flat else b

    def send_start(s, x, recv):
        slot = lax.rem(s, SENDS)
        recv[block_of(recv, f)] = send[slot, x, f]
        for d in partner_steps(fsdp_count):
            peer = along_fsdp(d)
            pltpu.make_async_remote_copy(
                src_ref=send.at[slot, x, peer],
                dst_ref=recv.at[block_of(recv, f)],
                send_sem=sent.at[slot, x],
                recv_sem=arrived.at[s, x],
                device_id=(peer, t),
                device_id_type=MESH,
            ).start()

    def exchanged():
        return send.at[0, 0, pl.ds(0, fsdp_count - 1)]

    def send_wait(s, x):
        pltpu.make_async_copy(exchanged(), exchanged(), sent.at[lax.rem(s, SENDS), x]).wait()

    def recv_wait(s, x):
        pltpu.make_async_copy(exchanged(), exchanged(), arrived.at[s, x]).wait()

    lines = block_rows // LANES
    square = (LANES, LANES)
    lane = lax.broadcasted_iota(jnp.int32, square, 1)
    sublane = lax.broadcasted_iota(jnp.int32, square, 0)

    def across(column):
        return jnp.broadcast_to(column, square)

    def turned(row):
        return jnp.transpose(across(row))

    def ones_where(mask):
        return jnp.where(mask, 1, 0)

    def inside(index):
        return jnp.clip(index, 0, block_rows - 1)

    def to_scalars(table, idx):
        copy = pltpu.make_async_copy(table, idx, table_sem)
        copy.start()
        copy.wait()

    def fill_send_idx():
        mine = [target_ref[pl.ds(f * lines + c, 1), :] for c in range(lines)]
        for c in range(lines):
            column, smaller = turned(mine[c]), jnp.zeros(square, jnp.int32)
            for row in mine:
                smaller = smaller + ones_where(row < column)
            spread[c] = across(jnp.sum(smaller, axis=1, keepdims=True))
        for c in range(lines):
            source = jnp.zeros(square, jnp.int32)
            for d in range(lines):
                source = source + jnp.where(spread[d] == c * LANES + lane, d * LANES + sublane, 0)
            send_table[pl.ds(c, 1), :] = inside(jnp.sum(source, axis=0, keepdims=True))
        to_scalars(send_table, send_idx)

    def fill_place_idx():
        def one_line(c, carry):
            wanted = f * block_rows + c * LANES + sublane

            def one_row(k, block):
                return block + jnp.where(target_ref[pl.ds(k, 1), :] == wanted, k // lines, 0)

            block = lax.fori_loop(
                0, target_ref.shape[0], one_row, jnp.zeros(square, jnp.int32), unroll=4
            )
            spread[c] = across(jnp.sum(block, axis=1, keepdims=True))
            place_table[pl.ds(c, 1), :] = jnp.transpose(spread[c])[:1]
            return carry

        lax.fori_loop(0, lines, one_line, 0)
        blocks = [place_table[pl.ds(c, 1), :] for c in range(lines)]
        for c in range(lines):
            column = spread[c]
            earlier = ones_where((blocks[c] == column) & (lane < sublane))
            for d in range(c):
                earlier = earlier + ones_where(blocks[d] == column)
            rank = jnp.sum(earlier, axis=1, keepdims=True)
            place_table[pl.ds(c, 1), :] = inside(jnp.transpose(column * pair + across(rank))[:1])
        to_scalars(place_table, place_idx)

    run = math.gcd(pair, UNROLL)

    def gather(s, x):
        slot = lax.rem(s, SENDS)

        def one_block(b, carry):
            def one_run(k, carry):
                at = b * pair + k * run
                line, column = at // LANES, at % LANES
                for u in range(run):
                    row = send_idx[line, column + u]
                    send[slot, x, b, pl.ds(k * run + u, 1), :] = stages[x][pl.ds(row, 1), :]
                return carry

            return lax.fori_loop(0, pair // run, one_run, carry)

        lax.fori_loop(0, fsdp_count, one_block, 0)

    def place(s, x, recv):
        def one_line(c, carry):
            def one_run(k, carry):
                for u in range(UNROLL):
                    index = place_idx[c, k * UNROLL + u]
                    if flat:
                        row = recv[pl.ds(index, 1), :]
                    else:
                        row = recv[index // pair, pl.ds(index % pair, 1), :]
                    out[x, s, pl.ds(c * LANES + k * UNROLL + u, 1), :] = row
                return carry

            return lax.fori_loop(0, LANES // UNROLL, one_run, carry)

        lax.fori_loop(0, lines, one_line, 0)

    tile = math.gcd(block_rows, 64)

    def adam(s):
        scale = scale_ref[...]

        def clipped_of(rows):
            return scale * grad[s, rows, :].astype(jnp.float32)

        adam_unit(clipped_of, step_ref, out.at[:, s], out.at[:, s])

    def keep_clipped():
        scale = scale_ref[...]

        def one_tile(k, carry):
            rows = pl.ds(pl.multiple_of(k * tile, tile), tile)
            out[3, steps - 1, rows, :] = scale * grad[steps - 1, rows, :].astype(jnp.float32)
            return carry

        lax.fori_loop(0, block_rows // tile, one_tile, 0)

    def square_sum():
        def one_unit(s, total):
            def one_tile(k, total):
                rows = pl.ds(pl.multiple_of(k * tile, tile), tile)
                wide = grad[s, rows, :].astype(jnp.float32)
                return total + wide * wide

            return lax.fori_loop(0, block_rows // tile, one_tile, total)

        total = lax.fori_loop(0, steps, one_unit, jnp.zeros((tile, LANES), jnp.float32))
        return jnp.sum(total, axis=0, keepdims=True)

    def partial_copies(which):
        if which == 0:
            peers = [(f, along_tp(d)) for d in range(1, tp_count)]
            source, target = partial, from_tp.at[t]
        else:
            peers = [(along_fsdp(d), t) for d in partner_steps(fsdp_count)]
            source, target = partial_row, from_fsdp.at[f]
        return [
            pltpu.make_async_remote_copy(
                src_ref=source,
                dst_ref=target,
                send_sem=partial_sems.at[2 * which],
                recv_sem=partial_sems.at[2 * which + 1],
                device_id=peer,
                device_id_type=MESH,
            )
            for peer in peers
        ]

    def partial_wait(which, side):
        held = (from_tp, from_fsdp)[which]
        members = (tp_count, fsdp_count)[which]
        if members > 1:
            whole = held.at[pl.ds(0, members - 1)]
            pltpu.make_async_copy(whole, whole, partial_sems.at[2 * which + side]).wait()

    def summed(held, members):
        total = held[0]
        for i in range(1, members):
            total = total + held[i]
        return total

    def grad_copy(s):
        return pltpu.make_async_copy(unit(grad_ref, 0, s), grad.at[s], grad_sem)

    def over_steps(body):
        lax.fori_loop(0, steps, lambda s, carry: (body(s), carry)[1], 0)

    barrier = pltpu.get_barrier_semaphore()
    partners = [(along_fsdp(d), t) for d in partner_steps(fsdp_count)]
    partners += [(f, along_tp(d)) for d in range(1, tp_count)]
    for peer in partners:
        pl.semaphore_signal(barrier, inc=1, device_id=peer, device_id_type=MESH)
    for x in range(3):
        stage_own(0, x).start()
    pl.semaphore_wait(barrier, len(partners))
    for x in range(3):
        tp_start(0, x, True)
    over_steps(lambda s: grad_copy(s).start())
    fill_send_idx()

    def begin_total():
        pltpu.make_async_copy(grad, grad, grad_sem).wait()
        own = square_sum()
        partial[...] = own
        from_tp[t] = own
        for copy in partial_copies(0):
            copy.start()

    def spread_total():
        partial_wait(0, 1)
        row = summed(from_tp, tp_count)
        partial_row[...] = row
        from_fsdp[f] = row
        for copy in partial_copies(1):
            copy.start()

    def end_total():
        partial_wait(1, 1)
        total = jnp.sum(summed(from_fsdp, fsdp_count), axis=1, keepdims=True)
        scale = jnp.minimum(1.0, math.sqrt(entries) / jnp.sqrt(total))
        scale_ref[...] = jnp.broadcast_to(scale, scale_ref.shape)
        keep_clipped()

    def step(s, carry):
        for x in range(3):

            @pl.when(s < steps)
            def _():
                stage_wait(s, x)
                pl.when(s >= SENDS)(lambda: send_wait(s - SENDS, x))
                gather(s, x)
                with_arrival(s, x, send_start)
                pl.when(s + 1 < steps)(lambda: tp_start(s + 1, x))
                if x == 0:
                    pl.when(s == 0)(begin_total)
                if x == 1:
                    pl.when(s == 0)(fill_place_idx)
                if x == 2:
                    pl.when(s == 0)(spread_total)
                after, y = (s, x + 1) if x < 2 else (s + 1, 0)

                @pl.when((after > 0) & (after < steps))
                def _():
                    tp_wait(after, y, tp_landed)
                    stage_start(after, y)

            @pl.when(s >= 1)
            def _():
                recv_wait(s - 1, x)
                with_arrival(s - 1, x, place)

        @pl.when(s >= 1)
        def _():
            pl.when(s == 1)(end_total)
            pl.when(s < steps)(lambda: adam(s - 1))

        return carry

    lax.fori_loop(0, steps + 1, step, 0)
    for x in range(3):
        for s in range(max(0, steps - SENDS), steps):
            send_wait(s, x)
        over_steps(lambda s: tp_wait(s, x, tp_sent))
    partial_wait(0, 0)
    partial_wait(1, 0)


def drain_kernel(step_ref, held, *refs):
    outs, (last, sem) = refs[:4], refs[4:]
    final = held.shape[1] - 1

    def copy(i, u):
        source = last.at[i] if u == final else held.at[i, u]
        return pltpu.make_async_copy(source, outs[i].at[:, u * LANES : (u + 1) * LANES], sem.at[i, u])

    earlier = [copy(i, u) for i in range(4) for u in range(final)]
    for one in earlier:
        one.start()
    adam_unit(lambda rows: held[3, final, rows, :], step_ref, held.at[:, final], last)
    latest = [copy(i, final) for i in range(4)]
    for one in latest:
        one.start()
    for one in earlier + latest:
        one.wait()


def per_device(entries, saved_master, saved_first, saved_second, grad, row_target, step):
    tp_count, fsdp_count = lax.axis_size("tp"), lax.axis_size("fsdp")
    block_rows, columns = grad.shape
    piece = saved_master.shape[0]
    lines = block_rows // LANES
    pair = block_rows // fsdp_count
    steps = columns // LANES

    def kernel(*refs):
        restore_kernel((tp_count, fsdp_count), entries, *refs)

    smem = pl.BlockSpec(memory_space=pltpu.SMEM)
    hbm = pl.BlockSpec(memory_space=pltpu.HBM)
    vmem = pl.BlockSpec(memory_space=pltpu.VMEM)
    dma = pltpu.SemaphoreType.DMA
    wide = jnp.float32
    blocks = (block_rows,) if pair % 8 == 0 else (fsdp_count, pair)
    arrival = pltpu.VMEM((*blocks, LANES), wide)
    held, _ = pl.pallas_call(
        kernel,
        out_shape=[
            pltpu.VMEM((4, steps, block_rows, LANES), wide),
            jax.ShapeDtypeStruct((steps, 3, tp_count, piece, LANES), wide),
        ],
        in_specs=[smem, vmem] + [hbm] * 4,
        out_specs=[vmem, hbm],
        scratch_shapes=[
            pltpu.SMEM((lines, LANES), jnp.int32),
            pltpu.SMEM((lines, LANES), jnp.int32),
            pltpu.VMEM((lines, LANES), jnp.int32),
            pltpu.VMEM((lines, LANES), jnp.int32),
            pltpu.VMEM((lines, LANES, LANES), jnp.int32),
            dma,
            pltpu.VMEM((tp_count * piece, LANES), wide),
            pltpu.VMEM((tp_count * piece, LANES), wide),
            pltpu.VMEM((tp_count * piece, LANES), wide),
            pltpu.VMEM((SENDS, 3, fsdp_count, pair, LANES), wide),
        ]
        + [arrival] * (3 * ARRIVALS)
        + [
            pltpu.VMEM((steps, block_rows, LANES), grad.dtype),
            pltpu.VMEM((1, LANES), wide),
            pltpu.VMEM((1, LANES), wide),
            pltpu.VMEM((tp_count, 1, LANES), wide),
            pltpu.VMEM((fsdp_count, 1, LANES), wide),
            pltpu.VMEM((1, LANES), wide),
            dma((steps, 3)),
            dma((steps, 3)),
            dma((3,)),
            dma((SENDS, 3)),
            dma((steps, 3)),
            dma,
            dma((4,)),
        ],
        compiler_params=pltpu.CompilerParams(
            has_side_effects=True, collective_id=0, vmem_limit_bytes=22 << 20
        ),
        name="restore",
    )(step, row_target.reshape(-1, LANES), saved_master, saved_first, saved_second, grad)

    out = jax.ShapeDtypeStruct((block_rows, columns), wide)
    return tuple(
        pl.pallas_call(
            drain_kernel,
            out_shape=[out] * 4,
            in_specs=[smem, vmem],
            out_specs=[hbm] * 4,
            scratch_shapes=[
                pltpu.VMEM((4, block_rows, LANES), wide),
                dma((4, steps)),
            ],
            compiler_params=pltpu.CompilerParams(vmem_limit_bytes=4 << 20),
            name="drain",
        )(step, held)
    )


def solution(mesh):
    in_specs = (
        P(("fsdp", "tp"), None),
        P(("fsdp", "tp"), None),
        P(("fsdp", "tp"), None),
        P("fsdp", "tp"),
        P(),
        P(),
    )
    out_specs = (P("fsdp", "tp"), P("fsdp", "tp"), P("fsdp", "tp"), P("fsdp", "tp"))

    def whole(saved_master, saved_first, saved_second, grad, row_target, step):
        def body(*args):
            return per_device(grad.shape[0] * grad.shape[1], *args)

        return jax.shard_map(
            body, mesh=mesh, in_specs=in_specs, out_specs=out_specs, check_vma=False
        )(saved_master, saved_first, saved_second, grad, row_target, step)

    return whole
```
